8 devices in a mesh: dp: 1 (over z), tp: 8 (over y, x, core).
Axes of the slice: x: 2, y: 2, z: 1, core: 2. Of those that a mesh axis runs over, the one named last changes fastest.
Arguments:
- tokens: int32 [48], P('dp')
- positions: int32 [48], P('dp')
- self_keys: bfloat16 [2, 48, 448, 8, 64], P(None, 'dp', None, 'tp')
- self_vals: bfloat16 [2, 48, 448, 8, 64], P(None, 'dp', None, 'tp')
- cross_keys: bfloat16 [2, 48, 1500, 8, 64], P(None, 'dp', None, 'tp')
- cross_vals: bfloat16 [2, 48, 1500, 8, 64], P(None, 'dp', None, 'tp')
- embed_table: bfloat16 [52224, 512], P('tp')
- pos_table: bfloat16 [448, 512], replicated
- w_qkv: bfloat16 [2, 512, 3, 8, 64], P(None, None, None, 'tp')
- w_cq: bfloat16 [2, 512, 8, 64], P(None, None, 'tp')
- in_bias: float32 [2, 3, 8, 64], P(None, None, 'tp')
- w_out: bfloat16 [2, 2, 8, 64, 512], P(None, None, 'tp')
- out_bias: float32 [2, 3, 512], replicated
- w_fc1: bfloat16 [2, 512, 2048], P(None, None, 'tp')
- b_fc1: float32 [2, 2048], P(None, 'tp')
- w_fc2: bfloat16 [2, 2048, 512], P(None, 'tp')
- ln_layers: float32 [2, 3, 2, 512], replicated
- ln_final: float32 [2, 512], replicated
Outputs:
- output 1: float32 [48, 52224], P('dp', 'tp')
- output 2: bfloat16 [2, 48, 448, 8, 64], P(None, 'dp', None, 'tp')
- output 3: bfloat16 [2, 48, 448, 8, 64], P(None, 'dp', None, 'tp')
All inputs are finite; a program needn't handle non-finite values.
Results may differ from the reference program's by a relative error of at most 0.012397.
Values are sent between devices in bfloat16 or wider.
A program may use at most 1 GiB of HBM per device.

```python
import jax
import jax.numpy as jnp
from jax import lax

SEQ_BATCH = 48
D_MODEL = 512
N_HEADS = 8
HEAD_DIM = 64
FF_DIM = 2048
VOCAB_SIZE = 51865
VOCAB_PAD = 52224
TEXT_CTX = 448
FRAMES = 1500
LAYERS = 2
FRAME_RANK = 8


def setup_inputs(seed: int = 0, part: int = 0) -> dict:
    base_key = jax.random.key(seed)
    part_keys = jax.random.split(jax.random.fold_in(base_key, part), 12)
    shared_keys = jax.random.split(jax.random.fold_in(base_key, 1000003), 14)

    def normal_draw(key_in, draw_shape, factor):
        return jax.random.normal(key_in, draw_shape, jnp.float32) * factor

    def structured(code_key, basis_key, noise_key, length, factor, noise_std):
        frame_codes = normal_draw(code_key, (SEQ_BATCH, length, FRAME_RANK), 1.0)
        code_basis = normal_draw(basis_key, (LAYERS, SEQ_BATCH, FRAME_RANK, N_HEADS, HEAD_DIM), factor * FRAME_RANK ** -0.5)
        mixed_rows = jnp.einsum('btr,lbrhe->lbthe', frame_codes, code_basis)
        return mixed_rows + normal_draw(noise_key, (LAYERS, SEQ_BATCH, length, N_HEADS, HEAD_DIM), noise_std)

    tokens = jax.random.randint(part_keys[0], (SEQ_BATCH,), 0, VOCAB_SIZE, dtype=jnp.int32)
    tokens = tokens.at[0].set(VOCAB_SIZE - 1).at[1].set(0)
    positions = jax.random.randint(part_keys[1], (SEQ_BATCH,), 0, TEXT_CTX, dtype=jnp.int32)
    positions = positions.at[0].set(TEXT_CTX - 1).at[1].set(0)
    self_keys = structured(part_keys[2], part_keys[3], part_keys[4], TEXT_CTX, 1.0, 0.3).astype(jnp.bfloat16)
    self_vals = structured(part_keys[2], part_keys[5], part_keys[6], TEXT_CTX, 1.0, 0.5).astype(jnp.bfloat16)
    cross_keys = structured(part_keys[7], part_keys[8], part_keys[9], FRAMES, 1.0, 0.3).astype(jnp.bfloat16)
    cross_vals = structured(part_keys[7], part_keys[10], part_keys[11], FRAMES, 1.0, 0.5).astype(jnp.bfloat16)
    embed_table = normal_draw(shared_keys[12], (VOCAB_PAD, D_MODEL), D_MODEL ** -0.25).astype(jnp.bfloat16)
    pos_table = normal_draw(shared_keys[13], (TEXT_CTX, D_MODEL), 0.5).astype(jnp.bfloat16)
    w_qkv = normal_draw(shared_keys[0], (LAYERS, D_MODEL, 3, N_HEADS, HEAD_DIM), D_MODEL ** -0.5).astype(jnp.bfloat16)
    w_cq = normal_draw(shared_keys[1], (LAYERS, D_MODEL, N_HEADS, HEAD_DIM), D_MODEL ** -0.5).astype(jnp.bfloat16)
    in_bias = normal_draw(shared_keys[2], (LAYERS, 3, N_HEADS, HEAD_DIM), 0.3)
    w_out = normal_draw(shared_keys[3], (LAYERS, 2, N_HEADS, HEAD_DIM, D_MODEL), D_MODEL ** -0.5).astype(jnp.bfloat16)
    out_bias = normal_draw(shared_keys[4], (LAYERS, 3, D_MODEL), 0.3)
    w_fc1 = normal_draw(shared_keys[5], (LAYERS, D_MODEL, FF_DIM), D_MODEL ** -0.5).astype(jnp.bfloat16)
    b_fc1 = normal_draw(shared_keys[6], (LAYERS, FF_DIM), 0.3)
    w_fc2 = normal_draw(shared_keys[7], (LAYERS, FF_DIM, D_MODEL), FF_DIM ** -0.5).astype(jnp.bfloat16)
    ln_layers = jnp.concatenate([1.0 + normal_draw(shared_keys[8], (LAYERS, 3, 1, D_MODEL), 0.2), normal_draw(shared_keys[9], (LAYERS, 3, 1, D_MODEL), 0.2)], axis=2)
    ln_final = jnp.concatenate([1.0 + normal_draw(shared_keys[10], (1, D_MODEL), 0.2), normal_draw(shared_keys[11], (1, D_MODEL), 0.2)], axis=0)
    return {'tokens': tokens, 'positions': positions, 'self_keys': self_keys, 'self_vals': self_vals, 'cross_keys': cross_keys, 'cross_vals': cross_vals, 'embed_table': embed_table, 'pos_table': pos_table, 'w_qkv': w_qkv, 'w_cq': w_cq, 'in_bias': in_bias, 'w_out': w_out, 'out_bias': out_bias, 'w_fc1': w_fc1, 'b_fc1': b_fc1, 'w_fc2': w_fc2, 'ln_layers': ln_layers, 'ln_final': ln_final}


def layer_norm(resid_in, ln_gain, ln_shift):
    row_mean = jnp.mean(resid_in, axis=-1, keepdims=True)
    centred = resid_in - row_mean
    variance = jnp.mean(centred * centred, axis=-1, keepdims=True)
    return (centred * lax.rsqrt(variance + 1e-5) * ln_gain + ln_shift).astype(jnp.bfloat16)


def attend(queries, key_rows, val_rows, mask_add):
    scores = jnp.einsum('bhe,bthe->bht', queries.astype(jnp.float32), key_rows.astype(jnp.float32)) * (HEAD_DIM ** -0.5) + mask_add
    weights = jax.nn.softmax(scores, axis=-1).astype(jnp.bfloat16)
    mixed_vals = jnp.einsum('bht,bthe->bhe', weights.astype(jnp.float32), val_rows.astype(jnp.float32))
    return mixed_vals.astype(jnp.bfloat16)


def project_out(attended, out_weight):
    summed = jnp.einsum('bhe,hed->bd', attended.astype(jnp.float32), out_weight.astype(jnp.float32))
    return summed.astype(jnp.bfloat16).astype(jnp.float32)


def reference(tokens, positions, self_keys, self_vals, cross_keys, cross_vals, embed_table, pos_table, w_qkv, w_cq, in_bias, w_out, out_bias, w_fc1, b_fc1, w_fc2, ln_layers, ln_final):
    residual = embed_table[tokens].astype(jnp.float32) + pos_table[positions].astype(jnp.float32)
    cache_pos = jnp.arange(TEXT_CTX)[None, :]
    write_mask = (cache_pos == positions[:, None])[:, :, None, None]
    self_mask = jnp.where(cache_pos <= positions[:, None], 0.0, -1e30)[:, None, :]

    def layer_body(resid_in, layer_args):
        (cache_keys, cache_vals, frame_keys, frame_vals, qkv_weight, cq_weight, bias_in, out_weight, bias_out, fc1_weight, fc1_bias, fc2_weight, ln_params) = layer_args
        hidden = layer_norm(resid_in, ln_params[0, 0], ln_params[0, 1])
        projected = jnp.einsum('bd,dthe->bthe', hidden.astype(jnp.float32), qkv_weight.astype(jnp.float32))
        queries = (projected[:, 0] + bias_in[0]).astype(jnp.bfloat16)
        key_new = projected[:, 1].astype(jnp.bfloat16)
        val_new = (projected[:, 2] + bias_in[1]).astype(jnp.bfloat16)
        keys_now = jnp.where(write_mask, key_new[:, None], cache_keys)
        vals_now = jnp.where(write_mask, val_new[:, None], cache_vals)
        resid_mid = resid_in + project_out(attend(queries, keys_now, vals_now, self_mask), out_weight[0]) + bias_out[0]
        hidden = layer_norm(resid_mid, ln_params[1, 0], ln_params[1, 1])
        cross_q = (jnp.einsum('bd,dhe->bhe', hidden.astype(jnp.float32), cq_weight.astype(jnp.float32)) + bias_in[2]).astype(jnp.bfloat16)
        resid_mid = resid_mid + project_out(attend(cross_q, frame_keys, frame_vals, 0.0), out_weight[1]) + bias_out[1]
        hidden = layer_norm(resid_mid, ln_params[2, 0], ln_params[2, 1])
        fc1_out = jnp.dot(hidden, fc1_weight, preferred_element_type=jnp.float32) + fc1_bias
        active = jax.nn.gelu(fc1_out, approximate=False).astype(jnp.bfloat16)
        fc2_out = jnp.dot(active, fc2_weight, preferred_element_type=jnp.float32).astype(jnp.bfloat16).astype(jnp.float32)
        resid_out = resid_mid + fc2_out + bias_out[2]
        return resid_out, (keys_now, vals_now)

    residual, new_caches = lax.scan(layer_body, residual, (self_keys, self_vals, cross_keys, cross_vals, w_qkv, w_cq, in_bias, w_out, out_bias, w_fc1, b_fc1, w_fc2, ln_layers))
    final_hidden = layer_norm(residual, ln_final[0], ln_final[1])
    logits = jnp.dot(final_hidden, embed_table.T, preferred_element_type=jnp.float32)
    return logits, new_caches[0], new_caches[1]
```

```python
import functools

import jax
import jax.numpy as jnp
from jax import lax
from jax.experimental import pallas as pl
from jax.experimental.pallas import tpu as pltpu
from jax.sharding import PartitionSpec as P

MESH = pl.DeviceIdType.MESH
BF = jnp.bfloat16
F32 = jnp.float32
NT = (((1,), (1,)), ((), ()))
N_DEV = 8
CHIP_PEERS = (2, 4, 6)


def dot(a, b):
    return jnp.dot(a, b, preferred_element_type=F32)


def dot_nt(a, b):
    return lax.dot_general(a, b, NT, preferred_element_type=F32)


def layer_norm(x, gain, shift):
    mean = jnp.mean(x, axis=-1, keepdims=True)
    centred = x - mean
    var = jnp.mean(centred * centred, axis=-1, keepdims=True)
    return (centred * lax.rsqrt(var + 1e-5) * gain + shift).astype(BF)


def gelu(x):
    return 0.5 * x * (1.0 + lax.erf(x * (0.5 ** 0.5)))


def chain_kernel(tok, pos, sk, sv, ck, cv, emb, ptab, wqkv, wcq, inb, wout, outb, wf1, bf1, wf2, lns, lnf,
                 kc, vc, e_v, fin,
                 cross, pt_v, wqkv_v, wcq_v, inb_v, outb_v, wf1_v, bf1_v, wf2_v, lns_v, lnf_v, wo_full,
                 rs_src, rs_dst, ag_buf, o_buf,
                 load_sem, kv_sem, cross_sem, wo_sem,
                 rs_s, rs_r, ag_s, ag_r, o_s, o_r, w_s, w_r):
    me = lax.axis_index('tp')
    n_seq, depth = fin.shape
    n_layers = kc.shape[0]
    n_blk = n_seq // 8
    chunk = n_seq // 2
    shard_rows = e_v.shape[0] * 8

    def local(src, dst, sem):
        cp = pltpu.make_async_copy(src, dst, sem)
        cp.start()
        return cp

    def remote(src, dst, s_sem, r_sem, k):
        return pltpu.make_async_remote_copy(src_ref=src, dst_ref=dst, send_sem=s_sem, recv_sem=r_sem,
                                            device_id={'tp': me ^ k}, device_id_type=MESH)

    names = [(ptab, pt_v), (emb, e_v), (lns, lns_v), (lnf, lnf_v), (inb, inb_v), (outb, outb_v), (bf1, bf1_v), (wqkv, wqkv_v)]
    bulk = [local(s, d, load_sem.at[i]) for i, (s, d) in enumerate(names)]
    wo_own = [local(wout.at[s // 2, s % 2], wo_full.at[s, me], wo_sem.at[s]) for s in range(4)]
    k_load = [local(sk.at[0], kc.at[0], kv_sem.at[0, 0]), None]
    v_load = [local(sv.at[0], vc.at[0], kv_sem.at[1, 0]), None]
    late = [local(s, d, load_sem.at[8 + i]) for i, (s, d) in enumerate([(wcq, wcq_v), (wf1, wf1_v), (wf2, wf2_v)])]
    ck_load = [local(ck.at[0], cross.at[0], cross_sem.at[0]), None]
    cv_load = [local(cv.at[0], cross.at[1], cross_sem.at[1]), None]
    k_load[1] = local(sk.at[1], kc.at[1], kv_sem.at[0, 1])
    v_load[1] = local(sv.at[1], vc.at[1], kv_sem.at[1, 1])
    ck_load[1] = local(ck.at[1], cross.at[2], cross_sem.at[2])
    cross_slot = ((0, 1), (2, 0))

    bar = pltpu.get_barrier_semaphore()
    for k in range(1, N_DEV):
        pl.semaphore_signal(bar, inc=1, device_id={'tp': me ^ k}, device_id_type=MESH)
    pl.semaphore_wait(bar, N_DEV - 1)

    pick_row = lax.broadcasted_iota(jnp.int32, (8, 64), 0)
    pick_lane = lax.broadcasted_iota(jnp.int32, (8, 64), 1)

    def pick_rows(table, index_of, ok_of):
        blocks = []
        for m in range(n_blk):
            groups = []
            want = jnp.full((8, 64), -1, jnp.int32)
            for j in range(8):
                i = index_of(8 * m + j)
                groups.append(table[lax.div(i, 8)].astype(F32))
                at = 8 * j + lax.rem(i, 8)
                if ok_of is not None:
                    at = jnp.where(ok_of(8 * m + j), at, -1)
                want = jnp.where(pick_row == j, at, want)
            one_hot = jnp.where(pick_lane == want, 1.0, 0.0).astype(BF)
            blocks.append(dot(one_hot, jnp.concatenate(groups, axis=0).astype(BF)))
        return jnp.concatenate(blocks, axis=0)

    def rs_start(ph, part):
        for p in range(N_DEV):
            rs_src[ph, p] = part[chunk * (p % 2):chunk * (p % 2) + chunk, 128 * (p // 2):128 * (p // 2) + 128]
        cps = [remote(rs_src.at[ph, me ^ k], rs_dst.at[ph, k], rs_s.at[ph, k], rs_r.at[ph, k], k) for k in range(1, N_DEV)]
        for cp in cps:
            cp.start()
        return cps

    def rs_finish(ph, cps):
        total = rs_src[ph, me]
        for k, cp in zip(range(1, N_DEV), cps):
            cp.wait_recv()
            total = total + rs_dst[ph, k]
        return total

    def ag_start(ph, piece):
        ag_buf[ph, me] = piece
        cps = [remote(ag_buf.at[ph, me], ag_buf.at[ph, me], ag_s.at[ph, k], ag_r.at[ph, k], k) for k in range(1, N_DEV)]
        for cp in cps:
            cp.start()
        return cps

    def ag_finish(ph, cps):
        for cp in cps:
            cp.wait_recv()
        cols = [jnp.concatenate([ag_buf[ph, 2 * c].astype(F32), ag_buf[ph, 2 * c + 1].astype(F32)], axis=0) for c in range(4)]
        return jnp.concatenate(cols, axis=1)

    def o_start(ph, o):
        o_buf[ph, me] = o
        cps = [remote(o_buf.at[ph, me], o_buf.at[ph, me], o_s.at[ph, k], o_r.at[ph, k], k) for k in range(1, N_DEV)]
        for cp in cps:
            cp.start()
        return cps

    lane128 = lax.broadcasted_iota(jnp.int32, (n_seq, 128), 1)

    def o_finish(ph, cps):
        for cp in cps:
            cp.wait_recv()
        pieces = [jnp.where(lane128 < 64, o_buf[ph, 2 * c].astype(F32), o_buf[ph, 2 * c + 1].astype(F32)) for c in range(4)]
        return jnp.concatenate(pieces, axis=1).astype(BF)

    def w_direct(s):
        wo_own[s].wait()
        cps = {k: remote(wo_full.at[s, me], wo_full.at[s, me], w_s.at[s, k], w_r.at[s, k], k) for k in (2, 4, 6, 1)}
        for cp in cps.values():
            cp.start()
        return cps

    def w_relay(s, cps):
        out = {}
        for k in CHIP_PEERS:
            cps[k].wait_recv()
            out[k ^ 1] = remote(wo_full.at[s, me ^ k], wo_full.at[s, me ^ k], w_s.at[s, k ^ 1], w_r.at[s, k ^ 1], 1)
            out[k ^ 1].start()
        return out

    def w_finish(s, cps, rel):
        cps[1].wait_recv()
        for cp in rel.values():
            cp.wait_recv()

    bulk[0].wait()
    pos_rows = pick_rows(pt_v, lambda b: pos[b], None)
    bulk[1].wait()
    first = me * shard_rows

    def owned(b):
        loc = tok[b] - first
        return jnp.logical_and(loc >= 0, loc < shard_rows)

    part = pick_rows(e_v, lambda b: jnp.clip(tok[b] - first, 0, shard_rows - 1), owned)
    cps0 = rs_start(0, part)
    w_cps = [w_direct(0), None, None, None]
    w_rel = [None] * 4
    piece = rs_finish(0, cps0)
    cps1 = ag_start(0, piece.astype(BF))
    w_cps[1] = w_direct(1)
    for cp in bulk[2:]:
        cp.wait()
    x = ag_finish(0, cps1) + pos_rows
    pending = cps0 + cps1

    blk_row = lax.broadcasted_iota(jnp.int32, (8, 8 * 64), 0)
    blk_lane = lax.broadcasted_iota(jnp.int32, (8, 8 * 64), 1)
    diag = blk_row == blk_lane // 64

    def spread(qd):
        return [jnp.where(diag, jnp.concatenate([qd[8 * m:8 * m + 8]] * 4, axis=1), 0.0).astype(BF) for m in range(n_blk)]

    def attend(qd, keys, vals, masks):
        lhs = spread(qd)
        outs = []
        weights = []
        for m in range(n_blk):
            kb = keys[8 * m:8 * m + 8]
            s = dot(lhs[m], kb.reshape(8 * 64, kb.shape[-1])) * 0.125
            if masks is not None:
                s = jnp.where(masks[m], s, -1e30)
            peak = jnp.max(s, axis=-1, keepdims=True)
            e = jnp.exp(s - peak)
            weights.append((e / jnp.sum(e, axis=-1, keepdims=True)).astype(BF))
        for m in range(n_blk):
            vb = vals[8 * m:8 * m + 8]
            r = jnp.where(diag, dot_nt(weights[m], vb.reshape(8 * 64, vb.shape[-1])), 0.0)
            y = (r[:, 0:128] + r[:, 128:256]) + (r[:, 256:384] + r[:, 384:512])
            outs.append(y + pltpu.roll(y, 64, 1))
        return jnp.concatenate(outs, axis=0).astype(BF)

    t_len = kc.shape[-1]
    t_lane = lax.broadcasted_iota(jnp.int32, (8, t_len), 1)
    t_row = lax.broadcasted_iota(jnp.int32, (8, t_len), 0)
    masks = []
    for m in range(n_blk):
        lim = jnp.zeros((8, t_len), jnp.int32)
        for j in range(8):
            lim = jnp.where(t_row == j, jnp.full((8, t_len), pos[8 * m + j], jnp.int32), lim)
        masks.append(t_lane <= lim)
    lane_t = lax.broadcasted_iota(jnp.int32, (64, t_len), 1)

    for l in range(n_layers):
        s_self, s_cross = 2 * l, 2 * l + 1
        h = layer_norm(x, lns_v[l, 0, 0:1], lns_v[l, 0, 1:2])
        wq, wk, wv = wqkv_v[l, 0], wqkv_v[l, 1], wqkv_v[l, 2]
        bq, bv = inb_v[l, 0], inb_v[l, 1]
        qd = (dot_nt(h, jnp.concatenate([wq, wq], axis=0)) + jnp.concatenate([bq, bq], axis=1)).astype(BF).astype(F32)
        kv = dot_nt(h, jnp.concatenate([wk, wv], axis=0)) + jnp.concatenate([jnp.zeros_like(bv), bv], axis=1)
        kv_t = kv.astype(BF).astype(F32).T
        k_load[l].wait()
        v_load[l].wait()
        for b in range(n_seq):
            hit = lane_t == pos[b]
            kcol = jnp.broadcast_to(kv_t[0:64, b:b + 1], (64, t_len)).astype(BF)
            vcol = jnp.broadcast_to(kv_t[64:128, b:b + 1], (64, t_len)).astype(BF)
            kc[l, b] = jnp.where(hit, kcol, kc[l, b])
            vc[l, b] = jnp.where(hit, vcol, vc[l, b])
        o = attend(qd, kc.at[l], vc.at[l], masks)
        cps = o_start(s_self, o)
        pending += cps
        w_rel[s_self] = w_relay(s_self, w_cps[s_self])
        if l == 0:
            w_cps[2] = w_direct(2)
            for cp in late:
                cp.wait()
        o_full = o_finish(s_self, cps)
        w_finish(s_self, w_cps[s_self], w_rel[s_self])
        x = x + dot(o_full, wo_full[s_self].reshape(N_DEV * 64, depth)).astype(BF).astype(F32) + outb_v[0, l:l + 1]
        h = layer_norm(x, lns_v[l, 1, 0:1], lns_v[l, 1, 1:2])
        wc, bc = wcq_v[l], inb_v[l, 2]
        qd = (dot_nt(h, jnp.concatenate([wc, wc], axis=0)) + jnp.concatenate([bc, bc], axis=1)).astype(BF).astype(F32)
        ck_load[l].wait()
        cv_load[l].wait()
        o = attend(qd, cross.at[cross_slot[l][0]], cross.at[cross_slot[l][1]], None)
        cps = o_start(s_cross, o)
        pending += cps
        w_rel[s_cross] = w_relay(s_cross, w_cps[s_cross])
        if l == 0:
            cv_load[1] = local(cv.at[1], cross.at[0], cross_sem.at[3])
            w_cps[3] = w_direct(3)
        o_full = o_finish(s_cross, cps)
        w_finish(s_cross, w_cps[s_cross], w_rel[s_cross])
        x = x + dot(o_full, wo_full[s_cross].reshape(N_DEV * 64, depth)).astype(BF).astype(F32) + outb_v[1, l:l + 1]
        h = layer_norm(x, lns_v[l, 2, 0:1], lns_v[l, 2, 1:2])
        act = gelu(dot(h, wf1_v[l]) + bf1_v[l:l + 1]).astype(BF)
        cps = rs_start(1 + l, dot(act, wf2_v[l]))
        piece = rs_finish(1 + l, cps)
        cps2 = ag_start(1 + l, piece.astype(BF))
        pending += cps + cps2
        x = x + ag_finish(1 + l, cps2) + outb_v[2, l:l + 1]
    fin[...] = layer_norm(x, lnf_v[0:1], lnf_v[1:2])
    for cp in pending:
        cp.wait_send()
    for s in range(4):
        for cp in w_cps[s].values():
            cp.wait_send()
        for cp in w_rel[s].values():
            cp.wait_send()


def head_kernel(kc, vc, e_v, fin, logits, nk, nv, out_v, sem, lsem):
    n_layers = kc.shape[0]
    cps = []
    for l in range(n_layers):
        for i, (s, d) in enumerate(((kc, nk), (vc, nv))):
            cp = pltpu.make_async_copy(s.at[l], d.at[l], sem.at[i, l])
            cp.start()
            cps.append(cp)
    h = fin[...]
    rows = e_v.shape[0]
    width = 384
    for c in range(rows // width):
        out_v[:, c * width:(c + 1) * width] = dot_nt(h, e_v[c * width:(c + 1) * width])
    cp = pltpu.make_async_copy(out_v, logits, lsem)
    cp.start()
    cp.wait()
    for cp in cps:
        cp.wait()


def solution(mesh):
    any_spec = pl.BlockSpec(memory_space=pl.ANY)
    vmem = pl.BlockSpec(memory_space=pltpu.VMEM)
    smem = pl.BlockSpec(memory_space=pltpu.SMEM)

    def hbm(a):
        return pltpu.with_memory_space_constraint(a, pltpu.HBM)

    def local_step(tokens, positions, self_keys, self_vals, cross_keys, cross_vals, embed_table, pos_table, w_qkv, w_cq, in_bias, w_out, out_bias, w_fc1, b_fc1, w_fc2, ln_layers, ln_final):
        n_layers, n_seq, t_len = self_keys.shape[:3]
        frames = cross_keys.shape[2]
        depth = embed_table.shape[1]

        def cols(c):
            return jnp.transpose(c, (0, 1, 3, 4, 2)).reshape(n_layers, n_seq, 64, c.shape[2])

        args = [cols(self_keys), cols(self_vals), cols(cross_keys), cols(cross_vals), embed_table.reshape(-1, 8, depth), pos_table.reshape(-1, 8, depth),
                jnp.transpose(w_qkv, (0, 2, 3, 4, 1)).reshape(n_layers, 3, 64, depth),
                jnp.transpose(w_cq, (0, 2, 3, 1)).reshape(n_layers, 64, depth),
                in_bias, w_out.reshape(n_layers, 2, 64, depth), jnp.transpose(out_bias, (1, 0, 2)),
                w_fc1, b_fc1, w_fc2, ln_layers, ln_final]
        hidden = w_fc1.shape[2]
        dma = pltpu.SemaphoreType.DMA
        kc, vc, e_v, fin = pl.pallas_call(
            chain_kernel,
            out_shape=(pltpu.VMEM((n_layers, n_seq, 64, t_len), BF), pltpu.VMEM((n_layers, n_seq, 64, t_len), BF),
                       pltpu.VMEM((embed_table.shape[0] // 8, 8, depth), BF), pltpu.VMEM((n_seq, depth), BF)),
            in_specs=[smem, smem] + [any_spec] * len(args),
            out_specs=(vmem, vmem, vmem, vmem),
            scratch_shapes=[
                pltpu.VMEM((3, n_seq, 64, frames), BF),
                pltpu.VMEM((pos_table.shape[0] // 8, 8, depth), BF),
                pltpu.VMEM((n_layers, 3, 64, depth), BF),
                pltpu.VMEM((n_layers, 64, depth), BF),
                pltpu.VMEM(in_bias.shape, F32),
                pltpu.VMEM((3, n_layers, depth), F32),
                pltpu.VMEM((n_layers, depth, hidden), BF),
                pltpu.VMEM((n_layers, hidden), F32),
                pltpu.VMEM((n_layers, hidden, depth), BF),
                pltpu.VMEM(ln_layers.shape, F32),
                pltpu.VMEM(ln_final.shape, F32),
                pltpu.VMEM((2 * n_layers, N_DEV, 64, depth), BF),
                pltpu.VMEM((1 + n_layers, N_DEV, n_seq // 2, 128), F32),
                pltpu.VMEM((1 + n_layers, N_DEV, n_seq // 2, 128), F32),
                pltpu.VMEM((1 + n_layers, N_DEV, n_seq // 2, 128), BF),
                pltpu.VMEM((2 * n_layers, N_DEV, n_seq, 128), BF),
                dma((11,)), dma((2, n_layers)), dma((4,)), dma((2 * n_layers,)),
                dma((1 + n_layers, N_DEV)), dma((1 + n_layers, N_DEV)),
                dma((1 + n_layers, N_DEV)), dma((1 + n_layers, N_DEV)),
                dma((2 * n_layers, N_DEV)), dma((2 * n_layers, N_DEV)),
                dma((2 * n_layers, N_DEV)), dma((2 * n_layers, N_DEV)),
            ],
            compiler_params=pltpu.CompilerParams(collective_id=0, has_side_effects=True, vmem_limit_bytes=40 * 2 ** 20),
            name='chain',
        )(tokens, positions, *[hbm(a) for a in args])

        logits, nk, nv = pl.pallas_call(
            head_kernel,
            out_shape=(jax.ShapeDtypeStruct((n_seq, embed_table.shape[0]), F32),
                       jax.ShapeDtypeStruct(kc.shape, BF), jax.ShapeDtypeStruct(vc.shape, BF)),
            in_specs=[vmem] * 4,
            out_specs=(any_spec, any_spec, any_spec),
            scratch_shapes=[pltpu.VMEM((n_seq, embed_table.shape[0]), F32), dma((2, n_layers)), dma],
            compiler_params=pltpu.CompilerParams(vmem_limit_bytes=40 * 2 ** 20),
            name='head',
        )(*[pltpu.with_memory_space_constraint(a, pltpu.VMEM) for a in (kc, vc, e_v.reshape(embed_table.shape), fin)])

        def uncols(c):
            return jnp.transpose(c.reshape(n_layers, n_seq, 1, 64, t_len), (0, 1, 4, 2, 3))

        return logits, uncols(nk), uncols(nv)

    batch_spec = P('dp')
    cache_spec = P(None, 'dp', None, 'tp', None)
    in_specs = (batch_spec, batch_spec, cache_spec, cache_spec, cache_spec, cache_spec, P('tp', None), P(None, None), P(None, None, None, 'tp', None), P(None, None, 'tp', None), P(None, None, 'tp', None), P(None, None, 'tp', None, None), P(None, None, None), P(None, None, 'tp'), P(None, 'tp'), P(None, 'tp', None), P(None, None, None, None), P(None, None))
    out_specs = (P('dp', 'tp'), cache_spec, cache_spec)
    return jax.shard_map(local_step, mesh=mesh, in_specs=in_specs, out_specs=out_specs, check_vma=False)
```

```python
import functools

import jax
import jax.numpy as jnp
from jax import lax
from jax.experimental import pallas as pl
from jax.experimental.pallas import tpu as pltpu
from jax.sharding import PartitionSpec as P

MESH = pl.DeviceIdType.MESH
BF = jnp.bfloat16
F32 = jnp.float32
NT = (((1,), (1,)), ((), ()))
N_DEV = 8
ROWS = 16
CHIP_PEERS = (2, 4, 6)


def dot(a, b):
    return jnp.dot(a, b, preferred_element_type=F32)


def dot_nt(a, b):
    return lax.dot_general(a, b, NT, preferred_element_type=F32)


def layer_norm(x, gain, shift):
    mean = jnp.mean(x, axis=-1, keepdims=True)
    centred = x - mean
    var = jnp.mean(centred * centred, axis=-1, keepdims=True)
    return (centred * lax.rsqrt(var + 1e-5) * gain + shift).astype(BF)


def gelu(x):
    return 0.5 * x * (1.0 + lax.erf(x * (0.5 ** 0.5)))


def chain_kernel(tok_h, pos_h, sk, sv, ck, cv, emb, ptab, wqkv, wcq, inb, wout, outb, wf1, bf1, wf2, lns, lnf,
                 kc, vc, e_v, fin,
                 tok, pos, cross, pt_v, wqkv_v, wcq_v, inb_v, outb_v, wf1_v, bf1_v, wf2_v, lns_v, lnf_v, wo_full,
                 emb_buf, rs_src, rs_dst, ag_buf, o_buf,
                 load_sem, kv_sem, cross_sem, wo_sem,
                 e_s, e_r, rs_s, rs_r, ag_s, ag_r, o_s, o_r, w_s, w_r):
    me = lax.axis_index('tp')
    n_seq, depth = fin.shape
    n_layers = kc.shape[0]
    groups = n_seq // ROWS
    g_blk = ROWS // 8
    shard_rows = e_v.shape[0] * 8
    t_len = kc.shape[-1]

    def local(src, dst, sem):
        cp = pltpu.make_async_copy(src, dst, sem)
        cp.start()
        return cp

    sends = []

    def exchange(src_of, dst_of, s_sem, r_sem, peers=tuple(range(1, N_DEV))):
        cps = {}
        for k in peers:
            cp = pltpu.make_async_remote_copy(src_ref=src_of(k), dst_ref=dst_of(k), send_sem=s_sem(k), recv_sem=r_sem(k),
                                              device_id={'tp': me ^ k}, device_id_type=MESH)
            cp.start()
            cps[k] = cp
            sends.append(cp)
        return cps

    def arrived(cps):
        for cp in cps.values():
            cp.wait_recv()

    scalars = [local(tok_h, tok, load_sem.at[0]), local(pos_h, pos, load_sem.at[1])]
    wo_own = [local(wout.at[0, 0], wo_full.at[0, me], wo_sem.at[0])]
    tables = [local(emb, e_v, load_sem.at[2]), local(ptab, pt_v, load_sem.at[3])]
    small = [(lns, lns_v), (lnf, lnf_v), (inb, inb_v), (outb, outb_v), (bf1, bf1_v), (wqkv, wqkv_v)]
    small = [local(s, d, load_sem.at[4 + i]) for i, (s, d) in enumerate(small)]
    k_load = [local(sk.at[0], kc.at[0], kv_sem.at[0, 0]), None]
    v_load = [local(sv.at[0], vc.at[0], kv_sem.at[1, 0]), None]
    wo_own += [local(wout.at[s // 2, s % 2], wo_full.at[s, me], wo_sem.at[s]) for s in range(1, 4)]
    late = [local(s, d, load_sem.at[10 + i]) for i, (s, d) in enumerate([(wcq, wcq_v), (wf1, wf1_v), (wf2, wf2_v)])]
    ck_load = [local(ck.at[0], cross.at[0], cross_sem.at[0]), None]
    cv_load = [local(cv.at[0], cross.at[1], cross_sem.at[1]), None]
    k_load[1] = local(sk.at[1], kc.at[1], kv_sem.at[0, 1])
    v_load[1] = local(sv.at[1], vc.at[1], kv_sem.at[1, 1])
    ck_load[1] = local(ck.at[1], cross.at[2], cross_sem.at[2])
    cross_slot = ((0, 1), (2, 0))

    bar = pltpu.get_barrier_semaphore()
    for k in range(1, N_DEV):
        pl.semaphore_signal(bar, inc=1, device_id={'tp': me ^ k}, device_id_type=MESH)
    pl.semaphore_wait(bar, N_DEV - 1)

    w_cps = [None] * 4
    w_rel = [None] * 4

    def w_direct(s):
        wo_own[s].wait()
        w_cps[s] = exchange(lambda k: wo_full.at[s, me], lambda k: wo_full.at[s, me],
                            lambda k: w_s.at[s, k], lambda k: w_r.at[s, k], (2, 4, 6, 1))

    def w_relay(s):
        w_rel[s] = []
        for k in CHIP_PEERS:
            w_cps[s][k].wait_recv()
            cp = pltpu.make_async_remote_copy(src_ref=wo_full.at[s, me ^ k], dst_ref=wo_full.at[s, me ^ k],
                                              send_sem=w_s.at[s, k ^ 1], recv_sem=w_r.at[s, k ^ 1],
                                              device_id={'tp': me ^ 1}, device_id_type=MESH)
            cp.start()
            w_rel[s].append(cp)
            sends.append(cp)

    def w_finish(s):
        w_cps[s][1].wait_recv()
        for cp in w_rel[s]:
            cp.wait_recv()

    w_direct(0)

    pick_row = lax.broadcasted_iota(jnp.int32, (8, 64), 0)
    pick_lane = lax.broadcasted_iota(jnp.int32, (8, 64), 1)

    def pick_rows(table, g, index_of, ok_of):
        blocks = []
        for m in range(g_blk):
            rows = []
            want = jnp.full((8, 64), -1, jnp.int32)
            for j in range(8):
                b = ROWS * g + 8 * m + j
                i = index_of(b)
                rows.append(table[lax.div(i, 8)].astype(F32))
                at = 8 * j + lax.rem(i, 8)
                if ok_of is not None:
                    at = jnp.where(ok_of(b), at, -1)
                want = jnp.where(pick_row == j, at, want)
            one_hot = jnp.where(pick_lane == want, 1.0, 0.0).astype(BF)
            blocks.append(dot(one_hot, jnp.concatenate(rows, axis=0).astype(BF)))
        return jnp.concatenate(blocks, axis=0)

    first = me * shard_rows

    def owned(b):
        loc = tok[b] - first
        return jnp.logical_and(loc >= 0, loc < shard_rows)

    for cp in scalars:
        cp.wait()
    tables[0].wait()
    emb_cps = []
    for g in range(groups):
        emb_buf[g, me] = pick_rows(e_v, g, lambda b: jnp.clip(tok[b] - first, 0, shard_rows - 1), owned).astype(BF)
        emb_cps.append(exchange(lambda k: emb_buf.at[g, me], lambda k: emb_buf.at[g, me], lambda k: e_s.at[g, k], lambda k: e_r.at[g, k]))
    tables[1].wait()
    pos_rows = [pick_rows(pt_v, g, lambda b: pos[b], None) for g in range(groups)]
    for cp in small:
        cp.wait()

    diag = lax.broadcasted_iota(jnp.int32, (8, 8 * 64), 0) == lax.broadcasted_iota(jnp.int32, (8, 8 * 64), 1) // 64
    lane128 = lax.broadcasted_iota(jnp.int32, (ROWS, 128), 1)
    t_lane = lax.broadcasted_iota(jnp.int32, (8, t_len), 1)
    t_row = lax.broadcasted_iota(jnp.int32, (8, t_len), 0)
    lane_t = lax.broadcasted_iota(jnp.int32, (64, t_len), 1)
    limits = []
    for m in range(n_seq // 8):
        lim = jnp.zeros((8, t_len), jnp.int32)
        for j in range(8):
            lim = jnp.where(t_row == j, pos[8 * m + j], lim)
        limits.append(lim)

    def scores(qd, m, keys):
        lhs = jnp.where(diag, jnp.concatenate([qd[8 * m:8 * m + 8]] * 4, axis=1), 0.0).astype(BF)
        return dot(lhs, keys.reshape(8 * 64, keys.shape[-1])) * 0.125

    def mix(w, vals):
        r = jnp.where(diag, dot_nt(w, vals.reshape(8 * 64, vals.shape[-1])), 0.0)
        y = (r[:, 0:128] + r[:, 128:256]) + (r[:, 256:384] + r[:, 384:512])
        return y + pltpu.roll(y, 64, 1)

    def o_start(s, g, o):
        o_buf[s, g, me] = o.astype(BF)
        i = s * groups + g
        return exchange(lambda k: o_buf.at[s, g, me], lambda k: o_buf.at[s, g, me], lambda k: o_s.at[i, k], lambda k: o_r.at[i, k])

    def o_finish(s, g, cps):
        arrived(cps)
        pieces = [jnp.where(lane128 < 64, o_buf[s, g, 2 * c].astype(F32), o_buf[s, g, 2 * c + 1].astype(F32)) for c in range(4)]
        o_full = jnp.concatenate(pieces, axis=1).astype(BF)
        return dot(o_full, wo_full[s].reshape(N_DEV * 64, depth)).astype(BF).astype(F32)

    half = ROWS // 2

    def rs_start(l, g, part):
        for p in range(N_DEV):
            rs_src[l, g, p] = part[half * (p % 2):half * (p % 2) + half, 128 * (p // 2):128 * (p // 2) + 128]
        i = l * groups + g
        return exchange(lambda k: rs_src.at[l, g, me ^ k], lambda k: rs_dst.at[l, g, k], lambda k: rs_s.at[i, k], lambda k: rs_r.at[i, k])

    def ag_start(l, g, cps):
        arrived(cps)
        total = rs_src[l, g, me]
        for k in range(1, N_DEV):
            total = total + rs_dst[l, g, k]
        ag_buf[l, g, me] = total.astype(BF)
        i = l * groups + g
        return exchange(lambda k: ag_buf.at[l, g, me], lambda k: ag_buf.at[l, g, me], lambda k: ag_s.at[i, k], lambda k: ag_r.at[i, k])

    def ag_finish(l, g, cps):
        arrived(cps)
        cols = [jnp.concatenate([ag_buf[l, g, 2 * c].astype(F32), ag_buf[l, g, 2 * c + 1].astype(F32)], axis=0) for c in range(4)]
        return jnp.concatenate(cols, axis=1)

    def self_stage(l, g, x):
        h = layer_norm(x, lns_v[l, 0, 0:1], lns_v[l, 0, 1:2])
        wq, wk, wv = wqkv_v[l, 0], wqkv_v[l, 1], wqkv_v[l, 2]
        bq, bv = inb_v[l, 0], inb_v[l, 1]
        qd = (dot_nt(h, jnp.concatenate([wq, wq], axis=0)) + jnp.concatenate([bq, bq], axis=1)).astype(BF).astype(F32)
        kv = dot_nt(h, jnp.concatenate([wk, wv], axis=0)) + jnp.concatenate([jnp.zeros_like(bv), bv], axis=1)
        kv = kv.astype(BF).astype(F32)
        vd = jnp.where(lane128 < 64, pltpu.roll(kv, 64, 1), kv)
        new_score = jnp.sum(jnp.where(lane128 < 64, qd * kv, 0.0), axis=-1, keepdims=True) * 0.125
        if g == 0:
            k_load[l].wait()
            v_load[l].wait()
        outs = []
        for m in range(g_blk):
            lim = limits[g * g_blk + m]
            rows = pl.ds(ROWS * g + 8 * m, 8)
            sn = new_score[8 * m:8 * m + 8]
            sc = jnp.where(t_lane < lim, scores(qd, m, kc[l, rows]), -1e30)
            peak = jnp.maximum(jnp.max(sc, axis=-1, keepdims=True), sn)
            e = jnp.exp(sc - peak)
            en = jnp.exp(sn - peak)
            den = jnp.sum(e, axis=-1, keepdims=True) + en
            w_new = (en / den).astype(BF).astype(F32)
            outs.append(mix((e / den).astype(BF), vc[l, rows]) + w_new * vd[8 * m:8 * m + 8])
        return o_start(2 * l, g, jnp.concatenate(outs, axis=0)), kv

    def patch(l, g, kv):
        kv_t = kv.T
        for j in range(ROWS):
            b = ROWS * g + j
            hit = lane_t == pos[b]
            kcol = jnp.broadcast_to(kv_t[0:64, j:j + 1], (64, t_len)).astype(BF)
            vcol = jnp.broadcast_to(kv_t[64:128, j:j + 1], (64, t_len)).astype(BF)
            kc[l, b] = jnp.where(hit, kcol, kc[l, b])
            vc[l, b] = jnp.where(hit, vcol, vc[l, b])

    def cross_stage(l, g, x, cps):
        x = x + o_finish(2 * l, g, cps) + outb_v[0, l:l + 1]
        h = layer_norm(x, lns_v[l, 1, 0:1], lns_v[l, 1, 1:2])
        wc, bc = wcq_v[l], inb_v[l, 2]
        qd = (dot_nt(h, jnp.concatenate([wc, wc], axis=0)) + jnp.concatenate([bc, bc], axis=1)).astype(BF).astype(F32)
        if g == 0:
            ck_load[l].wait()
            cv_load[l].wait()
        ks, vs = cross_slot[l]
        weights = []
        for m in range(g_blk):
            sc = scores(qd, m, cross[ks, pl.ds(ROWS * g + 8 * m, 8)])
            e = jnp.exp(sc - jnp.max(sc, axis=-1, keepdims=True))
            weights.append((e / jnp.sum(e, axis=-1, keepdims=True)).astype(BF))
        outs = [mix(weights[m], cross[vs, pl.ds(ROWS * g + 8 * m, 8)]) for m in range(g_blk)]
        return x, o_start(2 * l + 1, g, jnp.concatenate(outs, axis=0))

    def mlp_stage(l, g, x, cps):
        x = x + o_finish(2 * l + 1, g, cps) + outb_v[1, l:l + 1]
        h = layer_norm(x, lns_v[l, 2, 0:1], lns_v[l, 2, 1:2])
        act = gelu(dot(h, wf1_v[l]) + bf1_v[l:l + 1]).astype(BF)
        return x, rs_start(l, g, dot(act, wf2_v[l]))

    x = [None] * groups
    cps = emb_cps
    for l in range(n_layers):
        kvs = []
        for g in range(groups):
            if l == 0:
                arrived(cps[g])
                total = emb_buf[g, 0].astype(F32)
                for p in range(1, N_DEV):
                    total = total + emb_buf[g, p].astype(F32)
                x[g] = total + pos_rows[g]
                if g == 0:
                    w_relay(0)
            else:
                x[g] = x[g] + ag_finish(l - 1, g, cps[g]) + outb_v[2, l - 1:l]
            cps[g], kv = self_stage(l, g, x[g])
            kvs.append(kv)
        if l == 0:
            w_direct(1)
        else:
            w_relay(3)
        for g in range(groups):
            patch(l, g, kvs[g])
        w_finish(2 * l)
        if l == 0:
            for cp in late:
                cp.wait()
        for g in range(groups):
            x[g], cps[g] = cross_stage(l, g, x[g], cps[g])
            if l == 0 and g == 1:
                w_relay(1)
        if l == 0:
            cv_load[1] = local(cv.at[1], cross.at[0], cross_sem.at[3])
            w_direct(2)
        w_finish(2 * l + 1)
        for g in range(groups):
            x[g], cps[g] = mlp_stage(l, g, x[g], cps[g])
        if l == 0:
            w_relay(2)
            w_direct(3)
        cps = [ag_start(l, g, cps[g]) for g in range(groups)]
    for g in range(groups):
        x[g] = x[g] + ag_finish(n_layers - 1, g, cps[g]) + outb_v[2, n_layers - 1:n_layers]
        fin[ROWS * g:ROWS * g + ROWS] = layer_norm(x[g], lnf_v[0:1], lnf_v[1:2])
    for cp in sends:
        cp.wait_send()


def head_kernel(kc, vc, e_v, fin, logits, nk, nv, out_v, sem, lsem):
    n_layers = kc.shape[0]
    cps = []
    for l in range(n_layers):
        for i, (s, d) in enumerate(((kc, nk), (vc, nv))):
            cp = pltpu.make_async_copy(s.at[l], d.at[l], sem.at[i, l])
            cp.start()
            cps.append(cp)
    h = fin[...]
    rows = e_v.shape[0]
    width = 384
    for c in range(rows // width):
        out_v[:, c * width:(c + 1) * width] = dot_nt(h, e_v[c * width:(c + 1) * width])
    cp = pltpu.make_async_copy(out_v, logits, lsem)
    cp.start()
    cp.wait()
    for cp in cps:
        cp.wait()


def solution(mesh):
    any_spec = pl.BlockSpec(memory_space=pl.ANY)
    vmem = pl.BlockSpec(memory_space=pltpu.VMEM)

    def hbm(a):
        return pltpu.with_memory_space_constraint(a, pltpu.HBM)

    def local_step(tokens, positions, self_keys, self_vals, cross_keys, cross_vals, embed_table, pos_table, w_qkv, w_cq, in_bias, w_out, out_bias, w_fc1, b_fc1, w_fc2, ln_layers, ln_final):
        n_layers, n_seq, t_len = self_keys.shape[:3]
        frames = cross_keys.shape[2]
        depth = embed_table.shape[1]

        def cols(c):
            return jnp.transpose(c, (0, 1, 3, 4, 2)).reshape(n_layers, n_seq, 64, c.shape[2])

        args = [cols(self_keys), cols(self_vals), cols(cross_keys), cols(cross_vals), embed_table.reshape(-1, 8, depth), pos_table.reshape(-1, 8, depth),
                jnp.transpose(w_qkv, (0, 2, 3, 4, 1)).reshape(n_layers, 3, 64, depth),
                jnp.transpose(w_cq, (0, 2, 3, 1)).reshape(n_layers, 64, depth),
                in_bias, w_out.reshape(n_layers, 2, 64, depth), jnp.transpose(out_bias, (1, 0, 2)),
                w_fc1, b_fc1, w_fc2, ln_layers, ln_final]
        hidden = w_fc1.shape[2]
        groups = n_seq // ROWS
        dma = pltpu.SemaphoreType.DMA
        kc, vc, e_v, fin = pl.pallas_call(
            chain_kernel,
            out_shape=(pltpu.VMEM((n_layers, n_seq, 64, t_len), BF), pltpu.VMEM((n_layers, n_seq, 64, t_len), BF),
                       pltpu.VMEM((embed_table.shape[0] // 8, 8, depth), BF), pltpu.VMEM((n_seq, depth), BF)),
            in_specs=[any_spec] * (2 + len(args)),
            out_specs=(vmem, vmem, vmem, vmem),
            scratch_shapes=[
                pltpu.SMEM((n_seq,), jnp.int32), pltpu.SMEM((n_seq,), jnp.int32),
                pltpu.VMEM((3, n_seq, 64, frames), BF),
                pltpu.VMEM((pos_table.shape[0] // 8, 8, depth), BF),
                pltpu.VMEM((n_layers, 3, 64, depth), BF),
                pltpu.VMEM((n_layers, 64, depth), BF),
                pltpu.VMEM(in_bias.shape, F32),
                pltpu.VMEM((3, n_layers, depth), F32),
                pltpu.VMEM((n_layers, depth, hidden), BF),
                pltpu.VMEM((n_layers, hidden), F32),
                pltpu.VMEM((n_layers, hidden, depth), BF),
                pltpu.VMEM(ln_layers.shape, F32),
                pltpu.VMEM(ln_final.shape, F32),
                pltpu.VMEM((2 * n_layers, N_DEV, 64, depth), BF),
                pltpu.VMEM((groups, N_DEV, ROWS, depth), BF),
                pltpu.VMEM((n_layers, groups, N_DEV, ROWS // 2, 128), F32),
                pltpu.VMEM((n_layers, groups, N_DEV, ROWS // 2, 128), F32),
                pltpu.VMEM((n_layers, groups, N_DEV, ROWS // 2, 128), BF),
                pltpu.VMEM((2 * n_layers, groups, N_DEV, ROWS, 128), BF),
                dma((13,)), dma((2, n_layers)), dma((4,)), dma((2 * n_layers,)),
                dma((groups, N_DEV)), dma((groups, N_DEV)),
                dma((n_layers * groups, N_DEV)), dma((n_layers * groups, N_DEV)),
                dma((n_layers * groups, N_DEV)), dma((n_layers * groups, N_DEV)),
                dma((2 * n_layers * groups, N_DEV)), dma((2 * n_layers * groups, N_DEV)),
                dma((2 * n_layers, N_DEV)), dma((2 * n_layers, N_DEV)),
            ],
            compiler_params=pltpu.CompilerParams(collective_id=0, has_side_effects=True, vmem_limit_bytes=40 * 2 ** 20),
            name='chain',
        )(tokens, positions, *[hbm(a) for a in args])

        logits, nk, nv = pl.pallas_call(
            head_kernel,
            out_shape=(jax.ShapeDtypeStruct((n_seq, embed_table.shape[0]), F32),
                       jax.ShapeDtypeStruct(kc.shape, BF), jax.ShapeDtypeStruct(vc.shape, BF)),
            in_specs=[vmem] * 4,
            out_specs=(any_spec, any_spec, any_spec),
            scratch_shapes=[pltpu.VMEM((n_seq, embed_table.shape[0]), F32), dma((2, n_layers)), dma],
            compiler_params=pltpu.CompilerParams(vmem_limit_bytes=40 * 2 ** 20),
            name='head',
        )(*[pltpu.with_memory_space_constraint(a, pltpu.VMEM) for a in (kc, vc, e_v.reshape(embed_table.shape), fin)])

        def uncols(c):
            return jnp.transpose(c.reshape(n_layers, n_seq, 1, 64, t_len), (0, 1, 4, 2, 3))

        return logits, uncols(nk), uncols(nv)

    batch_spec = P('dp')
    cache_spec = P(None, 'dp', None, 'tp', None)
    in_specs = (batch_spec, batch_spec, cache_spec, cache_spec, cache_spec, cache_spec, P('tp', None), P(None, None), P(None, None, None, 'tp', None), P(None, None, 'tp', None), P(None, None, 'tp', None), P(None, None, 'tp', None, None), P(None, None, None), P(None, None, 'tp'), P(None, 'tp'), P(None, 'tp', None), P(None, None, None, None), P(None, None))
    out_specs = (P('dp', 'tp'), cache_spec, cache_spec)
    return jax.shard_map(local_step, mesh=mesh, in_specs=in_specs, out_specs=out_specs, check_vma=False)
```

```python
import functools

import jax
import jax.numpy as jnp
from jax import lax
from jax.experimental import pallas as pl
from jax.experimental.pallas import tpu as pltpu
from jax.sharding import PartitionSpec as P

MESH = pl.DeviceIdType.MESH
BF = jnp.bfloat16
F32 = jnp.float32
NT = (((1,), (1,)), ((), ()))
N_DEV = 8
ROWS = 16
CHIP_PEERS = (2, 4, 6)


def dot(a, b):
    return jnp.dot(a, b, preferred_element_type=F32)


def dot_nt(a, b):
    return lax.dot_general(a, b, NT, preferred_element_type=F32)


def layer_norm(x, gain, shift):
    mean = jnp.mean(x, axis=-1, keepdims=True)
    centred = x - mean
    var = jnp.mean(centred * centred, axis=-1, keepdims=True)
    return (centred * lax.rsqrt(var + 1e-5) * gain + shift).astype(BF)


def gelu(x):
    return 0.5 * x * (1.0 + lax.erf(x * (0.5 ** 0.5)))


def chain_kernel(tok_h, pos_h, sk, sv, ck, cv, emb, ptab, wqkv, wcq, inb, wout, outb, wf1, bf1, wf2, lns, lnf,
                 kc, vc, e_v, fin,
                 tok, pos, cross, pt_v, wqkv_v, wcq_v, inb_v, outb_v, wf1_v, bf1_v, wf2_v, lns_v, lnf_v, wo_full,
                 emb_buf, rs_src, rs_dst, ag_buf, o_buf,
                 load_sem, kv_sem, cross_sem, wo_sem,
                 e_s, e_r, rs_s, rs_r, ag_s, ag_r, o_s, o_r, w_s, w_r):
    me = lax.axis_index('tp')
    n_seq, depth = fin.shape
    n_layers = kc.shape[0]
    groups = n_seq // ROWS
    g_blk = ROWS // 8
    shard_rows = e_v.shape[0] * 8
    t_len = kc.shape[-1]

    def local(src, dst, sem):
        cp = pltpu.make_async_copy(src, dst, sem)
        cp.start()
        return cp

    def exchange(src_of, dst_of, s_sem, r_sem, peers=tuple(range(1, N_DEV))):
        for k in peers:
            pltpu.make_async_remote_copy(src_ref=src_of(k), dst_ref=dst_of(k), send_sem=s_sem, recv_sem=r_sem,
                                         device_id={'tp': me ^ k}, device_id_type=MESH).start()

    def arrived(buf, sem):
        pltpu.make_async_copy(buf, buf, sem).wait()

    scalars = [local(tok_h, tok, load_sem.at[0]), local(pos_h, pos, load_sem.at[1])]
    wo_own = [local(wout.at[0, 0], wo_full.at[0, me], wo_sem.at[0])]
    tables = [local(emb, e_v, load_sem.at[2]), local(ptab, pt_v, load_sem.at[3])]
    small = [(lns, lns_v), (lnf, lnf_v), (inb, inb_v), (outb, outb_v), (bf1, bf1_v), (wqkv, wqkv_v)]
    small = [local(s, d, load_sem.at[4 + i]) for i, (s, d) in enumerate(small)]
    k_load = [local(sk.at[0], kc.at[0], kv_sem.at[0, 0]), None]
    v_load = [local(sv.at[0], vc.at[0], kv_sem.at[1, 0]), None]
    wo_own += [local(wout.at[s // 2, s % 2], wo_full.at[s, me], wo_sem.at[s]) for s in range(1, 4)]
    late = [local(s, d, load_sem.at[10 + i]) for i, (s, d) in enumerate([(wcq, wcq_v), (wf1, wf1_v), (wf2, wf2_v)])]
    ck_load = [local(ck.at[0], cross.at[0], cross_sem.at[0]), None]
    cv_load = [local(cv.at[0], cross.at[1], cross_sem.at[1]), None]
    k_load[1] = local(sk.at[1], kc.at[1], kv_sem.at[0, 1])
    v_load[1] = local(sv.at[1], vc.at[1], kv_sem.at[1, 1])
    ck_load[1] = local(ck.at[1], cross.at[2], cross_sem.at[2])
    cross_slot = ((0, 1), (2, 0))

    bar = pltpu.get_barrier_semaphore()
    for k in range(1, N_DEV):
        pl.semaphore_signal(bar, inc=1, device_id={'tp': me ^ k}, device_id_type=MESH)
    pl.semaphore_wait(bar, N_DEV - 1)

    def w_direct(s):
        wo_own[s].wait()
        exchange(lambda k: wo_full.at[s, me], lambda k: wo_full.at[s, me], w_s, w_r.at[0, s], CHIP_PEERS)
        exchange(lambda k: wo_full.at[s, me], lambda k: wo_full.at[s, me], w_s, w_r.at[1, s], (1,))

    def w_relay(s):
        arrived(wo_full.at[s, 0:3], w_r.at[0, s])
        for k in CHIP_PEERS:
            exchange(lambda _: wo_full.at[s, me ^ k], lambda _: wo_full.at[s, me ^ k], w_s, w_r.at[1, s], (1,))

    def w_finish(s):
        arrived(wo_full.at[s, 0:4], w_r.at[1, s])

    w_direct(0)

    pick_row = lax.broadcasted_iota(jnp.int32, (8, 64), 0)
    pick_lane = lax.broadcasted_iota(jnp.int32, (8, 64), 1)

    def pick_rows(table, g, index_of, ok_of):
        blocks = []
        for m in range(g_blk):
            rows = []
            want = jnp.full((8, 64), -1, jnp.int32)
            for j in range(8):
                b = ROWS * g + 8 * m + j
                i = index_of(b)
                rows.append(table[lax.div(i, 8)].astype(F32))
                at = 8 * j + lax.rem(i, 8)
                if ok_of is not None:
                    at = jnp.where(ok_of(b), at, -1)
                want = jnp.where(pick_row == j, at, want)
            one_hot = jnp.where(pick_lane == want, 1.0, 0.0).astype(BF)
            blocks.append(dot(one_hot, jnp.concatenate(rows, axis=0).astype(BF)))
        return jnp.concatenate(blocks, axis=0)

    first = me * shard_rows

    def owned(b):
        loc = tok[b] - first
        return jnp.logical_and(loc >= 0, loc < shard_rows)

    for cp in scalars:
        cp.wait()
    tables[0].wait()
    for g in range(groups):
        emb_buf[g, me] = pick_rows(e_v, g, lambda b: jnp.clip(tok[b] - first, 0, shard_rows - 1), owned).astype(BF)
        exchange(lambda k: emb_buf.at[g, me], lambda k: emb_buf.at[g, me], e_s, e_r.at[g])
    tables[1].wait()
    pos_rows = [pick_rows(pt_v, g, lambda b: pos[b], None) for g in range(groups)]
    for cp in small:
        cp.wait()

    diag = lax.broadcasted_iota(jnp.int32, (8, 8 * 64), 0) == lax.broadcasted_iota(jnp.int32, (8, 8 * 64), 1) // 64
    lane128 = lax.broadcasted_iota(jnp.int32, (ROWS, 128), 1)
    t_lane = lax.broadcasted_iota(jnp.int32, (8, t_len), 1)
    t_row = lax.broadcasted_iota(jnp.int32, (8, t_len), 0)
    lane_t = lax.broadcasted_iota(jnp.int32, (64, t_len), 1)
    limits = []
    for m in range(n_seq // 8):
        lim = jnp.zeros((8, t_len), jnp.int32)
        for j in range(8):
            lim = jnp.where(t_row == j, pos[8 * m + j], lim)
        limits.append(lim)

    def scores(qd, m, keys):
        lhs = jnp.where(diag, jnp.concatenate([qd[8 * m:8 * m + 8]] * 4, axis=1), 0.0).astype(BF)
        return dot(lhs, keys.reshape(8 * 64, keys.shape[-1])) * 0.125

    def mix(w, vals):
        r = jnp.where(diag, dot_nt(w, vals.reshape(8 * 64, vals.shape[-1])), 0.0)
        y = (r[:, 0:128] + r[:, 128:256]) + (r[:, 256:384] + r[:, 384:512])
        return y + pltpu.roll(y, 64, 1)

    def o_start(s, g, o):
        o_buf[s, g, me] = o.astype(BF)
        exchange(lambda k: o_buf.at[s, g, me], lambda k: o_buf.at[s, g, me], o_s, o_r.at[s * groups + g])

    def o_finish(s, g):
        arrived(o_buf.at[s, g, 0:N_DEV - 1], o_r.at[s * groups + g])
        pieces = [jnp.where(lane128 < 64, o_buf[s, g, 2 * c].astype(F32), o_buf[s, g, 2 * c + 1].astype(F32)) for c in range(4)]
        o_full = jnp.concatenate(pieces, axis=1).astype(BF)
        return dot(o_full, wo_full[s].reshape(N_DEV * 64, depth)).astype(BF).astype(F32)

    half = ROWS // 2

    def rs_start(l, g, part):
        for p in range(N_DEV):
            rs_src[l, g, p] = part[half * (p % 2):half * (p % 2) + half, 128 * (p // 2):128 * (p // 2) + 128]
        exchange(lambda k: rs_src.at[l, g, me ^ k], lambda k: rs_dst.at[l, g, k], rs_s, rs_r.at[l * groups + g])

    def ag_start(l, g):
        arrived(rs_dst.at[l, g, 1:N_DEV], rs_r.at[l * groups + g])
        total = rs_src[l, g, me]
        for k in range(1, N_DEV):
            total = total + rs_dst[l, g, k]
        ag_buf[l, g, me] = total.astype(BF)
        exchange(lambda k: ag_buf.at[l, g, me], lambda k: ag_buf.at[l, g, me], ag_s, ag_r.at[l * groups + g])

    def ag_finish(l, g):
        arrived(ag_buf.at[l, g, 0:N_DEV - 1], ag_r.at[l * groups + g])
        cols = [jnp.concatenate([ag_buf[l, g, 2 * c].astype(F32), ag_buf[l, g, 2 * c + 1].astype(F32)], axis=0) for c in range(4)]
        return jnp.concatenate(cols, axis=1)

    def self_stage(l, g, x):
        h = layer_norm(x, lns_v[l, 0, 0:1], lns_v[l, 0, 1:2])
        wq, wk, wv = wqkv_v[l, 0], wqkv_v[l, 1], wqkv_v[l, 2]
        bq, bv = inb_v[l, 0], inb_v[l, 1]
        qd = (dot_nt(h, jnp.concatenate([wq, wq], axis=0)) + jnp.concatenate([bq, bq], axis=1)).astype(BF).astype(F32)
        kv = dot_nt(h, jnp.concatenate([wk, wv], axis=0)) + jnp.concatenate([jnp.zeros_like(bv), bv], axis=1)
        kv = kv.astype(BF).astype(F32)
        vd = jnp.where(lane128 < 64, pltpu.roll(kv, 64, 1), kv)
        new_score = jnp.sum(jnp.where(lane128 < 64, qd * kv, 0.0), axis=-1, keepdims=True) * 0.125
        if g == 0:
            k_load[l].wait()
            v_load[l].wait()
        outs = []
        for m in range(g_blk):
            lim = limits[g * g_blk + m]
            rows = pl.ds(ROWS * g + 8 * m, 8)
            sn = new_score[8 * m:8 * m + 8]
            sc = jnp.where(t_lane < lim, scores(qd, m, kc[l, rows]), -1e30)
            peak = jnp.maximum(jnp.max(sc, axis=-1, keepdims=True), sn)
            e = jnp.exp(sc - peak)
            en = jnp.exp(sn - peak)
            den = jnp.sum(e, axis=-1, keepdims=True) + en
            w_new = (en / den).astype(BF).astype(F32)
            outs.append(mix((e / den).astype(BF), vc[l, rows]) + w_new * vd[8 * m:8 * m + 8])
        o_start(2 * l, g, jnp.concatenate(outs, axis=0))
        return kv

    def patch(l, g, kv):
        kv_t = kv.T
        for j in range(ROWS):
            b = ROWS * g + j
            hit = lane_t == pos[b]
            kcol = jnp.broadcast_to(kv_t[0:64, j:j + 1], (64, t_len)).astype(BF)
            vcol = jnp.broadcast_to(kv_t[64:128, j:j + 1], (64, t_len)).astype(BF)
            kc[l, b] = jnp.where(hit, kcol, kc[l, b])
            vc[l, b] = jnp.where(hit, vcol, vc[l, b])

    def cross_stage(l, g, x):
        x = x + o_finish(2 * l, g) + outb_v[0, l:l + 1]
        h = layer_norm(x, lns_v[l, 1, 0:1], lns_v[l, 1, 1:2])
        wc, bc = wcq_v[l], inb_v[l, 2]
        qd = (dot_nt(h, jnp.concatenate([wc, wc], axis=0)) + jnp.concatenate([bc, bc], axis=1)).astype(BF).astype(F32)
        if g == 0:
            ck_load[l].wait()
            cv_load[l].wait()
        ks, vs = cross_slot[l]
        weights = []
        for m in range(g_blk):
            sc = scores(qd, m, cross[ks, pl.ds(ROWS * g + 8 * m, 8)])
            e = jnp.exp(sc - jnp.max(sc, axis=-1, keepdims=True))
            weights.append((e / jnp.sum(e, axis=-1, keepdims=True)).astype(BF))
        outs = [mix(weights[m], cross[vs, pl.ds(ROWS * g + 8 * m, 8)]) for m in range(g_blk)]
        o_start(2 * l + 1, g, jnp.concatenate(outs, axis=0))
        return x

    def mlp_stage(l, g, x):
        x = x + o_finish(2 * l + 1, g) + outb_v[1, l:l + 1]
        h = layer_norm(x, lns_v[l, 2, 0:1], lns_v[l, 2, 1:2])
        act = gelu(dot(h, wf1_v[l]) + bf1_v[l:l + 1]).astype(BF)
        rs_start(l, g, dot(act, wf2_v[l]))
        return x

    x = [None] * groups
    for l in range(n_layers):
        kvs = []
        for g in range(groups):
            if l == 0:
                arrived(emb_buf.at[g, 0:N_DEV - 1], e_r.at[g])
                total = emb_buf[g, 0].astype(F32)
                for p in range(1, N_DEV):
                    total = total + emb_buf[g, p].astype(F32)
                x[g] = total + pos_rows[g]
                if g == 0:
                    w_relay(0)
            else:
                x[g] = x[g] + ag_finish(l - 1, g) + outb_v[2, l - 1:l]
            kvs.append(self_stage(l, g, x[g]))
        if l == 0:
            w_direct(1)
        else:
            w_relay(3)
        for g in range(groups):
            patch(l, g, kvs[g])
        w_finish(2 * l)
        if l == 0:
            for cp in late:
                cp.wait()
        for g in range(groups):
            x[g] = cross_stage(l, g, x[g])
            if l == 0 and g == 1:
                w_relay(1)
        if l == 0:
            cv_load[1] = local(cv.at[1], cross.at[0], cross_sem.at[3])
            w_direct(2)
        w_finish(2 * l + 1)
        for g in range(groups):
            x[g] = mlp_stage(l, g, x[g])
        if l == 0:
            w_relay(2)
            w_direct(3)
        for g in range(groups):
            ag_start(l, g)
    for g in range(groups):
        x[g] = x[g] + ag_finish(n_layers - 1, g) + outb_v[2, n_layers - 1:n_layers]
        fin[ROWS * g:ROWS * g + ROWS] = layer_norm(x[g], lnf_v[0:1], lnf_v[1:2])
    arrived(emb_buf.at[:, 0:N_DEV - 1], e_s)
    arrived(o_buf.at[:, :, 0:N_DEV - 1], o_s)
    arrived(rs_src.at[:, :, 0:N_DEV - 1], rs_s)
    arrived(ag_buf.at[:, :, 0:N_DEV - 1], ag_s)
    arrived(wo_full.at[:, 0:N_DEV - 1], w_s)


def head_kernel(kc, vc, e_v, fin, logits, nk, nv, out_v, sem, lsem):
    n_layers = kc.shape[0]
    cps = []
    for l in range(n_layers):
        for i, (s, d) in enumerate(((kc, nk), (vc, nv))):
            cp = pltpu.make_async_copy(s.at[l], d.at[l], sem.at[i, l])
            cp.start()
            cps.append(cp)
    h = fin[...]
    rows = e_v.shape[0]
    width = 384
    for c in range(rows // width):
        out_v[:, c * width:(c + 1) * width] = dot_nt(h, e_v[c * width:(c + 1) * width])
    cp = pltpu.make_async_copy(out_v, logits, lsem)
    cp.start()
    cp.wait()
    for cp in cps:
        cp.wait()


def solution(mesh):
    any_spec = pl.BlockSpec(memory_space=pl.ANY)
    vmem = pl.BlockSpec(memory_space=pltpu.VMEM)

    def hbm(a):
        return pltpu.with_memory_space_constraint(a, pltpu.HBM)

    def local_step(tokens, positions, self_keys, self_vals, cross_keys, cross_vals, embed_table, pos_table, w_qkv, w_cq, in_bias, w_out, out_bias, w_fc1, b_fc1, w_fc2, ln_layers, ln_final):
        n_layers, n_seq, t_len = self_keys.shape[:3]
        frames = cross_keys.shape[2]
        depth = embed_table.shape[1]

        def cols(c):
            return jnp.transpose(c, (0, 1, 3, 4, 2)).reshape(n_layers, n_seq, 64, c.shape[2])

        args = [cols(self_keys), cols(self_vals), cols(cross_keys), cols(cross_vals), embed_table.reshape(-1, 8, depth), pos_table.reshape(-1, 8, depth),
                jnp.transpose(w_qkv, (0, 2, 3, 4, 1)).reshape(n_layers, 3, 64, depth),
                jnp.transpose(w_cq, (0, 2, 3, 1)).reshape(n_layers, 64, depth),
                in_bias, w_out.reshape(n_layers, 2, 64, depth), jnp.transpose(out_bias, (1, 0, 2)),
                w_fc1, b_fc1, w_fc2, ln_layers, ln_final]
        hidden = w_fc1.shape[2]
        groups = n_seq // ROWS
        dma = pltpu.SemaphoreType.DMA
        kc, vc, e_v, fin = pl.pallas_call(
            chain_kernel,
            out_shape=(pltpu.VMEM((n_layers, n_seq, 64, t_len), BF), pltpu.VMEM((n_layers, n_seq, 64, t_len), BF),
                       pltpu.VMEM((embed_table.shape[0] // 8, 8, depth), BF), pltpu.VMEM((n_seq, depth), BF)),
            in_specs=[any_spec] * (2 + len(args)),
            out_specs=(vmem, vmem, vmem, vmem),
            scratch_shapes=[
                pltpu.SMEM((n_seq,), jnp.int32), pltpu.SMEM((n_seq,), jnp.int32),
                pltpu.VMEM((3, n_seq, 64, frames), BF),
                pltpu.VMEM((pos_table.shape[0] // 8, 8, depth), BF),
                pltpu.VMEM((n_layers, 3, 64, depth), BF),
                pltpu.VMEM((n_layers, 64, depth), BF),
                pltpu.VMEM(in_bias.shape, F32),
                pltpu.VMEM((3, n_layers, depth), F32),
                pltpu.VMEM((n_layers, depth, hidden), BF),
                pltpu.VMEM((n_layers, hidden), F32),
                pltpu.VMEM((n_layers, hidden, depth), BF),
                pltpu.VMEM(ln_layers.shape, F32),
                pltpu.VMEM(ln_final.shape, F32),
                pltpu.VMEM((2 * n_layers, N_DEV, 64, depth), BF),
                pltpu.VMEM((groups, N_DEV, ROWS, depth), BF),
                pltpu.VMEM((n_layers, groups, N_DEV, ROWS // 2, 128), F32),
                pltpu.VMEM((n_layers, groups, N_DEV, ROWS // 2, 128), F32),
                pltpu.VMEM((n_layers, groups, N_DEV, ROWS // 2, 128), BF),
                pltpu.VMEM((2 * n_layers, groups, N_DEV, ROWS, 128), BF),
                dma((13,)), dma((2, n_layers)), dma((4,)), dma((2 * n_layers,)),
                dma, dma((groups,)), dma, dma((n_layers * groups,)), dma, dma((n_layers * groups,)),
                dma, dma((2 * n_layers * groups,)), dma, dma((2, 2 * n_layers)),
            ],
            compiler_params=pltpu.CompilerParams(collective_id=0, has_side_effects=True, vmem_limit_bytes=40 * 2 ** 20),
            name='chain',
        )(tokens, positions, *[hbm(a) for a in args])

        logits, nk, nv = pl.pallas_call(
            head_kernel,
            out_shape=(jax.ShapeDtypeStruct((n_seq, embed_table.shape[0]), F32),
                       jax.ShapeDtypeStruct(kc.shape, BF), jax.ShapeDtypeStruct(vc.shape, BF)),
            in_specs=[vmem] * 4,
            out_specs=(any_spec, any_spec, any_spec),
            scratch_shapes=[pltpu.VMEM((n_seq, embed_table.shape[0]), F32), dma((2, n_layers)), dma],
            compiler_params=pltpu.CompilerParams(vmem_limit_bytes=40 * 2 ** 20),
            name='head',
        )(*[pltpu.with_memory_space_constraint(a, pltpu.VMEM) for a in (kc, vc, e_v.reshape(embed_table.shape), fin)])

        def uncols(c):
            return jnp.transpose(c.reshape(n_layers, n_seq, 1, 64, t_len), (0, 1, 4, 2, 3))

        return logits, uncols(nk), uncols(nv)

    batch_spec = P('dp')
    cache_spec = P(None, 'dp', None, 'tp', None)
    in_specs = (batch_spec, batch_spec, cache_spec, cache_spec, cache_spec, cache_spec, P('tp', None), P(None, None), P(None, None, None, 'tp', None), P(None, None, 'tp', None), P(None, None, 'tp', None), P(None, None, 'tp', None, None), P(None, None, None), P(None, None, 'tp'), P(None, 'tp'), P(None, 'tp', None), P(None, None, None, None), P(None, None))
    out_specs = (P('dp', 'tp'), cache_spec, cache_spec)
    return jax.shard_map(local_step, mesh=mesh, in_specs=in_specs, out_specs=out_specs, check_vma=False)
```
